32 devices in a mesh: ang: 8 (over z, x), tile: 4 (over y, core).
Axes of the slice: x: 2, y: 2, z: 4, core: 2. Of those that a mesh axis runs over, the one named last changes fastest.
Arguments:
- sinogram: float32 [2, 64, 2048], P(None, 'ang'), may hold values from -6 to 6
- ray_offsets: int32 [64, 256], P('ang'), may hold values from 0 to 2047
- merge_matrices: float32 [3, 2, 2, 256, 256], replicated, may hold values from -1 to 1.5, as said below
Outputs:
- reconstruction: float32 [2, 2048, 2048], P(None, 'ang')
The draws below stay inside these ranges and needn't reach their ends.
Inputs may be any that keep to these rules, and one draw needn't show every extreme that they name: merge_matrices[l, b, k] is zero outside the columns b * (96) to b * 96 + 256 / 2 + 31.
All inputs are finite; a program needn't handle non-finite values.
Results may differ from the reference program's by a relative error of at most 0.0003.
Values sent between devices are 32-bit elements; how exact they have to be, the bound alone decides.
A program may use at most 768 MiB of HBM per device.

```python
import math
import jax
import jax.numpy as jnp
from jax import lax

NPIX = 2048
ANG_DEV = 8
SLICES = 2
ANGLES = 64
R = 256
HALO = 32
LEVELS = 3
N_ANG = 8


def draw_merge_matrices(key, part):
    shape = (LEVELS, 2, 2, R, R)
    noise = jnp.clip(jax.random.normal(key, shape, jnp.float32), -4.0, 4.0)
    width = R // 2 + HALO
    fine = jnp.arange(R, dtype=jnp.float32)[None, :, None]
    coarse = jnp.arange(R, dtype=jnp.float32)[None, None, :]
    half_bit = jnp.arange(2, dtype=jnp.float32)[:, None, None]
    centre = half_bit * (R // 2) + 0.5 * fine
    kernel = jnp.maximum(0.0, 1.0 - jnp.abs(coarse - centre))
    low_col = half_bit * (R // 2 - HALO)
    inside = jnp.logical_and(coarse >= low_col, coarse < low_col + width).astype(jnp.float32)
    kernel = kernel[None, :, None, :, :]
    inside = inside[None, :, None, :, :]
    return inside * (0.5 * kernel + 0.5 * noise / math.sqrt(width))


def set_ends(values, stream_key, smallest, largest):
    longest = values.shape.index(max(values.shape))
    spots = []
    for shift in (0, 1):
        where = [jax.random.randint(jax.random.fold_in(stream_key, axis), (), 0, length) for axis, length in enumerate(values.shape)]
        where[longest] = (where[longest] + shift) % values.shape[longest]
        spots.append(tuple(where))
    return values.at[spots[0]].set(smallest).at[spots[1]].set(largest)


def level_of(own_key, dims, cuts, smallest, largest):
    def one(position, parts):
        draws = jax.random.uniform(jax.random.fold_in(jax.random.fold_in(own_key, 6), position), (parts,), jnp.float32, smallest / len(cuts), largest / len(cuts))
        return jnp.repeat(jnp.exp(draws), dims[position] // parts).reshape((-1,) + (1,) * (len(dims) - position - 1))

    gain = one(*cuts[0])
    for cut in cuts[1:]:
        gain = gain * one(*cut)
    return gain


def scatter_about(key, dims, scale, bound, pieces=(), kind=jnp.bfloat16):
    entries = jax.random.normal(key, dims, jnp.float32) * scale
    if len(pieces) > 0:
        entries = level_of(key, dims, pieces, -0.22, 0.18) * entries
    return jnp.clip(entries, min=-bound, max=bound).astype(kind)


def setup_inputs(seed: int = 0) -> dict:
    splits = jax.random.split(jax.random.key(seed), 4)
    sinogram = scatter_about(splits[0], (SLICES, ANGLES, NPIX), 1.0, 6.0, ((1, 8),), jnp.float32)
    ray_offsets = set_ends(jax.random.randint(splits[1], (ANGLES, R), 0, NPIX), jax.random.fold_in(splits[1], 1), 0, NPIX - 1).astype(jnp.int32)
    merge_matrices = draw_merge_matrices(jax.random.fold_in(splits[3], 71), 0)
    return dict(sinogram=sinogram, ray_offsets=ray_offsets, merge_matrices=merge_matrices)


def apply_rows(matrix, field):
    return jnp.einsum('rk,...kw->...rw', matrix, field, precision=lax.Precision.HIGHEST)

def smear_rows(sinogram, offsets, columns):
    slices = sinogram.shape[0]
    angles = sinogram.shape[1]
    bin_count = sinogram.shape[2]
    row_count = offsets.shape[1]
    blocks = angles // 8
    grouped = sinogram.reshape(slices, blocks, 8, bin_count).transpose(1, 0, 2, 3)
    grouped_offsets = offsets.reshape(blocks, 8, row_count)
    angle_ids = jnp.arange(8, dtype=jnp.int32)[:, None, None]

    def add_block(running, inputs):
        rows_block, offset_block = inputs
        bin_index = jnp.remainder(columns[None, None, :] + offset_block[:, :, None], bin_count).astype(jnp.int32)
        samples = rows_block[:, angle_ids, bin_index]
        return (running + lax.optimization_barrier(jnp.sum(samples, axis=1)), None)
    zeros_init = jnp.zeros((slices, row_count, columns.shape[0]), jnp.float32)
    running, _ = lax.scan(add_block, zeros_init, (grouped, grouped_offsets))
    return running / math.sqrt(angles)

def reference(sinogram, ray_offsets, merge_matrices):
    grouped = sinogram.reshape(SLICES, N_ANG, ANG_DEV, NPIX).transpose(1, 0, 2, 3)
    offsets_grouped = ray_offsets.reshape(N_ANG, ANG_DEV, R)
    columns = jnp.arange(NPIX, dtype=jnp.int32)
    partial_value = lax.map(lambda inputs: smear_rows(inputs[0], inputs[1], columns), (grouped, offsets_grouped))
    for level_num in range(LEVELS):
        half_span = 2 ** (LEVELS - 1 - level_num)
        shaped = partial_value.reshape(N_ANG // (2 * half_span), 2, half_span, SLICES, R, NPIX)
        lower = shaped[:, 0]
        upper = shaped[:, 1]
        mats = merge_matrices[level_num]
        new_lower = apply_rows(mats[0, 0], lower) + apply_rows(mats[0, 1], upper)
        new_upper = apply_rows(mats[1, 0], upper) + apply_rows(mats[1, 1], lower)
        partial_value = jnp.stack([new_lower, new_upper], axis=1).reshape(N_ANG, SLICES, R, NPIX)
    return partial_value.transpose(1, 0, 2, 3).reshape(SLICES, NPIX, NPIX)
```

```python
import functools
import math

import jax
import jax.numpy as jnp
from jax import lax
from jax.experimental import pallas as pl
from jax.experimental.pallas import tpu as pltpu
from jax.sharding import PartitionSpec as P

LANES = 128
SUBLANES = 8
PITCH = 3 * SUBLANES + 1
ROW_PITCH = SUBLANES + 1
UNROLL = 80
TOP = 32767.0


def split_bf16(value):
    high = value.astype(jnp.bfloat16)
    return high, (value - high.astype(jnp.float32)).astype(jnp.bfloat16)


def dot3(left, right):
    dot = functools.partial(jnp.dot, preferred_element_type=jnp.float32)
    return dot(left[0], right[0]) + (dot(left[0], right[1]) + dot(left[1], right[0]))


def fused_kernel(dims, sino_ref, offsets_ref, merge_ref, out_ref, field_in, index_in, index_smem, merges, table_ref, samples_ref,
                 weights_high, weights_low, in_sems, smem_sems, send_sems, recv_sems, swap_send, swap_recv):
    levels, angles, rows, bins = dims
    groups = 2**levels
    margin = rows // 8
    width = rows // 2 + margin
    half = bins // 2
    own = lax.axis_index("ang")
    seat = lax.axis_index("tile")
    core = lax.rem(seat, 2)
    bits = [lax.rem(lax.div(own, 2 ** (levels - 1 - level)), 2) for level in range(levels)]

    loads = [pltpu.make_async_copy(sino_ref.at[core], field_in.at[0, :, pl.ds(0, bins)], in_sems.at[0])]
    for level in range(levels):
        loads.append(pltpu.make_async_copy(merge_ref.at[level, bits[level]], merges.at[level], in_sems.at[1 + level]))
    for load in loads:
        load.start()

    barrier = pltpu.get_barrier_semaphore()
    far = list(range(2, groups, 2))
    peers = [{"ang": own ^ k} for k in [1] + far] + [{"tile": seat ^ 1}]
    for peer in peers:
        pl.semaphore_signal(barrier, inc=1, device_id=peer, device_id_type=pl.DeviceIdType.MESH)

    index_in[0] = jnp.bitwise_and(offsets_ref[...] + (bins - 1), bins - 1) ^ (LANES - 1)
    loads[0].wait()
    largest = jnp.max(jnp.abs(field_in[0, :, pl.ds(0, bins)]))
    field_in[0, :, pl.ds(bins, LANES)] = jnp.full((angles, LANES), 1.0, jnp.float32) * largest
    pl.semaphore_wait(barrier, len(peers))

    def sends(k, target, slot):
        return [
            pltpu.make_async_remote_copy(
                src_ref=buffer.at[k],
                dst_ref=buffer.at[slot],
                send_sem=send_sems.at[n, slot],
                recv_sem=recv_sems.at[n, slot],
                device_id={"ang": target},
                device_id_type=pl.DeviceIdType.MESH,
            )
            for n, buffer in enumerate((field_in, index_in))
        ]

    moves = {k: sends(0, own ^ k, k) for k in [1] + far}
    for k in [1] + far:
        for move in moves[k]:
            move.start()
    index_copy = pltpu.make_async_copy(index_in.at[0], index_smem.at[0], smem_sems.at[0])
    index_copy.start()

    def prepare(k):
        peak = field_in[k, :, pl.ds(bins, LANES)]
        scale = TOP / jnp.maximum(peak, 1e-30)
        blocks = bins // LANES
        coded = []
        for block in range(blocks):
            value = field_in[k, :, pl.ds(block * LANES, LANES)]
            coded.append((value * scale + (TOP + 1.5)).astype(jnp.int32))
        for block in range(blocks):
            upper = jnp.left_shift(coded[(block + blocks // 2) % blocks] - int(TOP + 1), 16)
            packed = jnp.bitwise_or(upper, coded[block])
            for place in (block, block + blocks):
                if place < PITCH - 1:
                    table_ref[pl.ds(k * angles * PITCH + place, angles, stride=PITCH), :] = packed

    reverse_lane = LANES - 1 - lax.broadcasted_iota(jnp.int32, (SUBLANES, LANES), 1)
    row0 = bits[0] * (rows // 2 - margin)
    unroll = math.gcd(width, UNROLL)
    samples_half = groups * width * ROW_PITCH

    def project(k):
        unit = field_in[k, :, pl.ds(bins, LANES)] * (1.0 / (TOP * math.sqrt(angles)))

        def by_rows(step, carry):
            for u in range(unroll):
                q = step * unroll + u
                total = None
                upper = None
                for a in range(angles):
                    code = index_smem[k, a, row0 + q]
                    turn = jnp.bitwise_and(code, LANES - 1)
                    base = jnp.right_shift(code, 7) + (k * angles + a) * PITCH
                    near = table_ref[pl.ds(base, SUBLANES), :]
                    next_ = table_ref[pl.ds(base + 1, SUBLANES), :]
                    moved = pltpu.roll(jnp.where(reverse_lane < turn, near, next_), turn, 1)
                    high = jnp.right_shift(moved, 16)
                    total = moved if a == 0 else total + moved
                    upper = high if a == 0 else upper + high
                lower = total - jnp.left_shift(upper, 16) - angles * int(TOP + 1)
                at = (k * width + q) * ROW_PITCH
                samples_ref[pl.ds(at, SUBLANES), :] = lower.astype(jnp.float32) * unit
                samples_ref[pl.ds(samples_half + at, SUBLANES), :] = upper.astype(jnp.float32) * unit
            return carry

        lax.fori_loop(0, width // unroll, by_rows, 0)

    def prepare_weights():
        for load in loads[1:]:
            load.wait()
        parts = None
        for level in range(levels - 1, -1, -1):
            matrices = [merges[level, m] for m in range(2)]
            if level == 0:
                matrices = [jnp.where(bits[0] == 1, m[:, rows - width:], m[:, :width]) for m in matrices]
            if parts is None:
                parts = matrices
            else:
                matrices = [split_bf16(m) for m in matrices]
                parts = [dot3(part, m) for part in [split_bf16(p) for p in parts] for m in matrices]
        flips = [int(format(k, f"0{levels}b")[::-1], 2) for k in range(groups)]
        whole = jnp.concatenate([parts[i] for i in flips], axis=1)
        weights_high[...], weights_low[...] = split_bf16(whole)

    prepare(0)
    index_copy.wait()
    project(0)
    prepare_weights()
    forwards = {}
    for k in [1] + far + [f ^ 1 for f in far]:
        arrived = moves[k] if k in moves else forwards[k]
        for move in arrived:
            move.wait_recv()
        if k in far:
            forwards[k ^ 1] = sends(k, own ^ 1, k ^ 1)
            for move in forwards[k ^ 1]:
                move.start()
        index_copy = pltpu.make_async_copy(index_in.at[k], index_smem.at[k], smem_sems.at[k])
        index_copy.start()
        prepare(k)
        index_copy.wait()
        project(k)

    depth = groups * width
    pairs = bins // (2 * LANES)

    def swap(n):
        at = pl.ds(pl.multiple_of(n * 2 * LANES, 2 * LANES), 2 * LANES)
        return pltpu.make_async_remote_copy(
            src_ref=out_ref.at[core, :, at],
            dst_ref=out_ref.at[core, :, at],
            send_sem=swap_send.at[n],
            recv_sem=swap_recv.at[n],
            device_id={"tile": seat ^ 1},
            device_id_type=pl.DeviceIdType.MESH,
        )

    def by_columns(n, carry):
        first = (n // (pairs // 2)) * samples_half + (n % (pairs // 2)) * 2
        parts = [samples_ref[pl.ds(first + i, depth, stride=ROW_PITCH), :] for i in range(2)]
        field = split_bf16(jnp.concatenate(parts, axis=1))
        total = dot3((weights_high[...], weights_low[...]), field)
        out_ref[core, :, pl.ds(pl.multiple_of(n * 2 * LANES, 2 * LANES), 2 * LANES)] = total

        @pl.when(n > 0)
        def _():
            swap(n - 1).start()

        return carry

    lax.fori_loop(0, pairs, by_columns, 0)
    swap(pairs - 1).start()
    for k in moves:
        for move in moves[k]:
            move.wait_send()
    for k in forwards:
        for move in forwards[k]:
            move.wait_send()
    for n in range(pairs):
        swap(n).wait()


def body(sinogram, ray_offsets, merge_matrices):
    slices, angles, bins = sinogram.shape
    rows = ray_offsets.shape[1]
    levels = merge_matrices.shape[0]
    groups = lax.axis_size("ang")
    assert slices == 2 and lax.axis_size("tile") % 2 == 0
    assert groups == 2**levels and angles == SUBLANES and bins == 2 * SUBLANES * LANES
    width = rows // 2 + rows // 8
    vmem = pl.BlockSpec(memory_space=pltpu.VMEM)
    anywhere = pl.BlockSpec(memory_space=pl.ANY)
    dma = pltpu.SemaphoreType.DMA
    return pl.pallas_call(
        functools.partial(fused_kernel, (levels, angles, rows, bins)),
        out_shape=jax.ShapeDtypeStruct((slices, rows, bins), jnp.float32),
        in_specs=[anywhere, vmem, anywhere],
        out_specs=vmem,
        scratch_shapes=[
            pltpu.VMEM((groups, angles, bins + LANES), jnp.float32),
            pltpu.VMEM((groups, angles, rows), jnp.int32),
            pltpu.SMEM((groups, angles, rows), jnp.int32),
            pltpu.VMEM((levels, 2, rows, rows), jnp.float32),
            pltpu.VMEM((groups * angles * PITCH, LANES), jnp.int32),
            pltpu.VMEM((2 * groups * width * ROW_PITCH, LANES), jnp.float32),
            pltpu.VMEM((rows, groups * width), jnp.bfloat16),
            pltpu.VMEM((rows, groups * width), jnp.bfloat16),
            dma((1 + levels,)),
            dma((groups,)),
            dma((2, groups)),
            dma((2, groups)),
            dma((bins // (2 * LANES),)),
            dma((bins // (2 * LANES),)),
        ],
        compiler_params=pltpu.CompilerParams(
            collective_id=0, has_side_effects=True, vmem_limit_bytes=48 * 1024 * 1024
        ),
    )(sinogram, ray_offsets, merge_matrices)


def solution(mesh):
    placed = (P(None, "ang", None), P("ang", None), P())
    return jax.shard_map(
        body, mesh=mesh, in_specs=placed, out_specs=P(None, "ang", None), check_vma=False
    )
```

```python
import functools
import math

import jax
import jax.numpy as jnp
from jax import lax
from jax.experimental import pallas as pl
from jax.experimental.pallas import tpu as pltpu
from jax.sharding import PartitionSpec as P

LANES = 128
SUBLANES = 8
PITCH = 3 * SUBLANES + 1
ROW_PITCH = SUBLANES + 1
TOP = 32767.0


def split_bf16(value):
    high = value.astype(jnp.bfloat16)
    return high, (value - high.astype(jnp.float32)).astype(jnp.bfloat16)


def dot3(left, right):
    dot = functools.partial(jnp.dot, preferred_element_type=jnp.float32)
    return dot(left[0], right[0]) + (dot(left[0], right[1]) + dot(left[1], right[0]))


def fused_kernel(dims, sino_ref, offsets_ref, merge_ref, out_ref, field_in, index_in, index_kept, index_smem, merges, table_ref, samples_ref,
                 weights_high, weights_low, in_sems, smem_sems, send_sems, recv_sems, swap_send, swap_recv):
    levels, angles, rows, bins = dims
    groups = 2**levels
    width = rows // 2 + rows // 8
    half = bins // 2
    own = lax.axis_index("ang")
    seat = lax.axis_index("tile")
    core = lax.rem(seat, 2)
    bits = [lax.rem(lax.div(own, 2 ** (levels - 1 - level)), 2) for level in range(levels)]

    loads = [pltpu.make_async_copy(sino_ref.at[core], field_in.at[0, :, pl.ds(0, bins)], in_sems.at[0])]
    for level in range(levels):
        loads.append(pltpu.make_async_copy(merge_ref.at[level, bits[level]], merges.at[level], in_sems.at[1 + level]))
    for load in loads:
        load.start()

    barrier = pltpu.get_barrier_semaphore()
    far = list(range(2, groups, 2))
    peers = [{"ang": own ^ k} for k in [1] + far] + [{"tile": seat ^ 1}]
    for peer in peers:
        pl.semaphore_signal(barrier, inc=1, device_id=peer, device_id_type=pl.DeviceIdType.MESH)

    index_in[0] = jnp.bitwise_and(offsets_ref[...] + (bins - 1), bins - 1) ^ (LANES - 1)
    loads[0].wait()
    largest = jnp.max(jnp.abs(field_in[0, :, pl.ds(0, bins)]))
    field_in[0, :, pl.ds(bins, LANES)] = jnp.full((angles, LANES), 1.0, jnp.float32) * largest
    pl.semaphore_wait(barrier, len(peers))

    def send(n, k, target, slot):
        buffer = (index_in, field_in)[n]
        return pltpu.make_async_remote_copy(
            src_ref=buffer.at[k],
            dst_ref=buffer.at[slot],
            send_sem=send_sems.at[n, slot],
            recv_sem=recv_sems.at[n, slot],
            device_id={"ang": target},
            device_id_type=pl.DeviceIdType.MESH,
        )

    for n in range(2):
        for k in [1] + far:
            send(n, 0, own ^ k, k).start()

    turn_point = groups // 2

    def group_at(place):
        near = jnp.where(place <= turn_point, 2 * place - 2, 2 * (place - turn_point) + 1)
        return jnp.where(place < 2, place, near)

    def receive(n, place):
        k = group_at(place)

        @pl.when(place > 0)
        def _():
            send(n, k, own, k).wait_recv()

        @pl.when(jnp.logical_and(place >= 2, place <= turn_point))
        def _():
            send(n, k, own ^ 1, k + 1).start()

        return k

    def hand_over(place, side):
        codes = index_in[receive(0, place)]
        codes = jnp.where(bits[0] == 1, codes[:, rows - width:], codes[:, :width])
        index_kept[side] = codes + lax.broadcasted_iota(jnp.int32, codes.shape, 0) * (PITCH * LANES)
        index_copy(side).start()

    def index_copy(side):
        return pltpu.make_async_copy(index_kept.at[side], index_smem.at[side], smem_sems.at[side])

    def prepare(place, side):
        k = receive(1, place)
        peak = field_in[k, :, pl.ds(bins, LANES)]
        scale = TOP / jnp.maximum(peak, 1e-30)
        blocks = bins // LANES
        coded = []
        for block in range(blocks):
            value = field_in[k, :, pl.ds(block * LANES, LANES)]
            coded.append((value * scale + (TOP + 1.5)).astype(jnp.int32))
        for block in range(blocks):
            upper = jnp.left_shift(coded[(block + blocks // 2) % blocks] - int(TOP + 1), 16)
            packed = jnp.bitwise_or(upper, coded[block])
            for at in (block, block + blocks):
                if at < PITCH - 1:
                    table_ref[side, pl.ds(at, angles, stride=PITCH), :] = packed
        return peak * (1.0 / (TOP * math.sqrt(angles)))

    reverse_lane = LANES - 1 - lax.broadcasted_iota(jnp.int32, (SUBLANES, LANES), 1)
    samples_half = groups * width * ROW_PITCH

    def project(place, side, unit):
        start = place * (width * ROW_PITCH)
        for q in range(width):
            total = None
            upper = None
            for a in range(angles):
                code = index_smem[side, a, q]
                turn = jnp.bitwise_and(code, LANES - 1)
                base = jnp.right_shift(code, 7)
                near = table_ref[side, pl.ds(base, SUBLANES), :]
                next_ = table_ref[side, pl.ds(base + 1, SUBLANES), :]
                moved = pltpu.roll(jnp.where(reverse_lane < turn, near, next_), turn, 1)
                high = jnp.right_shift(moved, 16)
                total = moved if a == 0 else total + moved
                upper = high if a == 0 else upper + high
            lower = total - jnp.left_shift(upper, 16) - angles * int(TOP + 1)
            at = start + q * ROW_PITCH
            samples_ref[0, pl.ds(at, SUBLANES), :] = lower.astype(jnp.float32) * unit
            samples_ref[1, pl.ds(at, SUBLANES), :] = upper.astype(jnp.float32) * unit

    def prepare_weights():
        for load in loads[1:]:
            load.wait()
        parts = None
        for level in range(levels - 1, -1, -1):
            matrices = [merges[level, m] for m in range(2)]
            if level == 0:
                matrices = [jnp.where(bits[0] == 1, m[:, rows - width:], m[:, :width]) for m in matrices]
            if parts is None:
                parts = matrices
            else:
                matrices = [split_bf16(m) for m in matrices]
                parts = [dot3(part, m) for part in [split_bf16(p) for p in parts] for m in matrices]
        order = [0, 1] + far + [k ^ 1 for k in far]
        flips = [int(format(k, f"0{levels}b")[::-1], 2) for k in order]
        whole = jnp.concatenate([parts[i] for i in flips], axis=1)
        weights_high[...], weights_low[...] = split_bf16(whole)

    hand_over(0, 0)
    prepare_weights()

    def by_pairs(step, carry):
        place = 2 * step
        hand_over(place + 1, 1)
        unit = prepare(place, 0)
        index_copy(0).wait()
        project(place, 0, unit)

        @pl.when(place + 2 < groups)
        def _():
            hand_over(place + 2, 0)

        unit = prepare(place + 1, 1)
        index_copy(1).wait()
        project(place + 1, 1, unit)
        return carry

    lax.fori_loop(0, groups // 2, by_pairs, 0)

    depth = groups * width
    pairs = bins // (2 * LANES)

    def swap(n):
        at = pl.ds(pl.multiple_of(n * 2 * LANES, 2 * LANES), 2 * LANES)
        return pltpu.make_async_remote_copy(
            src_ref=out_ref.at[core, :, at],
            dst_ref=out_ref.at[core, :, at],
            send_sem=swap_send.at[n],
            recv_sem=swap_recv.at[n],
            device_id={"tile": seat ^ 1},
            device_id_type=pl.DeviceIdType.MESH,
        )

    def by_columns(n, carry):
        side = n // (pairs // 2)
        first = (n % (pairs // 2)) * 2
        parts = [samples_ref[side, pl.ds(first + i, depth, stride=ROW_PITCH), :] for i in range(2)]
        field = split_bf16(jnp.concatenate(parts, axis=1))
        total = dot3((weights_high[...], weights_low[...]), field)
        out_ref[core, :, pl.ds(pl.multiple_of(n * 2 * LANES, 2 * LANES), 2 * LANES)] = total

        @pl.when(n > 0)
        def _():
            swap(n - 1).start()

        return carry

    lax.fori_loop(0, pairs, by_columns, 0)
    swap(pairs - 1).start()
    for n in range(2):
        for k in range(1, groups):
            send(n, 0, own, k).wait_send()
    for n in range(pairs):
        swap(n).wait()


def body(sinogram, ray_offsets, merge_matrices):
    slices, angles, bins = sinogram.shape
    rows = ray_offsets.shape[1]
    levels = merge_matrices.shape[0]
    groups = lax.axis_size("ang")
    assert slices == 2 and lax.axis_size("tile") % 2 == 0
    assert groups == 2**levels and angles == SUBLANES and bins == 2 * SUBLANES * LANES
    width = rows // 2 + rows // 8
    vmem = pl.BlockSpec(memory_space=pltpu.VMEM)
    hbm = pl.BlockSpec(memory_space=pltpu.HBM)
    dma = pltpu.SemaphoreType.DMA
    return pl.pallas_call(
        functools.partial(fused_kernel, (levels, angles, rows, bins)),
        out_shape=pltpu.VMEM((slices, rows, bins), jnp.float32),
        in_specs=[hbm, vmem, hbm],
        out_specs=vmem,
        scratch_shapes=[
            pltpu.VMEM((groups, angles, bins + LANES), jnp.float32),
            pltpu.VMEM((groups, angles, rows), jnp.int32),
            pltpu.VMEM((2, angles, width), jnp.int32),
            pltpu.SMEM((2, angles, width), jnp.int32),
            pltpu.VMEM((levels, 2, rows, rows), jnp.float32),
            pltpu.VMEM((2, angles * PITCH, LANES), jnp.int32),
            pltpu.VMEM((2, groups * width * ROW_PITCH + SUBLANES, LANES), jnp.float32),
            pltpu.VMEM((rows, groups * width), jnp.bfloat16),
            pltpu.VMEM((rows, groups * width), jnp.bfloat16),
            dma((1 + levels,)),
            dma((2,)),
            dma((2, groups)),
            dma((2, groups)),
            dma((bins // (2 * LANES),)),
            dma((bins // (2 * LANES),)),
        ],
        compiler_params=pltpu.CompilerParams(
            collective_id=0, has_side_effects=True, vmem_limit_bytes=48 * 1024 * 1024
        ),
    )(*[pltpu.with_memory_space_constraint(x, pltpu.HBM) for x in (sinogram, ray_offsets, merge_matrices)])


def solution(mesh):
    placed = (P(None, "ang", None), P("ang", None), P())
    return jax.shard_map(
        body, mesh=mesh, in_specs=placed, out_specs=P(None, "ang", None), check_vma=False
    )
```

```python
import functools
import math

import jax
import jax.numpy as jnp
from jax import lax
from jax.experimental import pallas as pl
from jax.experimental.pallas import tpu as pltpu
from jax.sharding import PartitionSpec as P

LANES = 128
SUBLANES = 8
PITCH = 3 * SUBLANES + 1
ROW_PITCH = SUBLANES + 4
TOP = 32767.0


def split_bf16(value):
    high = value.astype(jnp.bfloat16)
    return high, (value - high.astype(jnp.float32)).astype(jnp.bfloat16)


def dot3(left, right):
    dot = functools.partial(jnp.dot, preferred_element_type=jnp.float32)
    return dot(left[0], right[0]) + (dot(left[0], right[1]) + dot(left[1], right[0]))


def fused_kernel(dims, sino_ref, offsets_ref, merge_ref, out_ref, field_in, index_in, index_smem, offsets, merges, table_ref,
                 samples_ref, weights_high, weights_low, in_sems, smem_sems, send_sems, recv_sems, ready_sem, swap_send, swap_recv):
    levels, angles, rows, bins = dims
    groups = 2**levels
    lines = groups // 2
    cuts = (rows // 2 - rows // 8, rows // 2 + rows // 8)
    width = cuts[1]
    own = lax.axis_index("ang")
    line, column = lax.div(own, 2), lax.rem(own, 2)
    seat = lax.axis_index("tile")
    core = lax.rem(seat, 2)
    bits = [lax.rem(lax.div(own, 2 ** (levels - 1 - level)), 2) for level in range(levels)]

    barrier = pltpu.get_barrier_semaphore()

    def greet(peer):
        pl.semaphore_signal(barrier, inc=1, device_id=peer, device_id_type=pl.DeviceIdType.MESH)

    greet({"ang": own ^ 1})
    greet({"tile": seat ^ 1})

    @pl.when(line > 0)
    def _():
        greet({"ang": own - 2})

    for step in range(1, lines):

        @pl.when(line + step < lines)
        def _():
            greet({"ang": own + 2 * step})

    loads = [
        pltpu.make_async_copy(sino_ref.at[core], field_in.at[own, :, pl.ds(0, bins)], in_sems.at[0]),
        pltpu.make_async_copy(offsets_ref, offsets, in_sems.at[1]),
    ]
    for level in range(levels):
        loads.append(pltpu.make_async_copy(merge_ref.at[level, bits[level]], merges.at[level], in_sems.at[2 + level]))
    for load in loads:
        load.start()
    loads[1].wait()
    place_code = lax.broadcasted_iota(jnp.int32, (angles, rows), 0) * (PITCH * LANES)
    codes = (jnp.bitwise_and(offsets[...] + (bins - 1), bins - 1) ^ (LANES - 1)) + place_code
    for part, (first, last) in enumerate(((0, cuts[0]), cuts, (cuts[1], rows))):
        index_in[own, :, pl.ds(part * LANES, last - first)] = codes[:, first:last]
    loads[0].wait()
    largest = jnp.max(jnp.abs(field_in[own, :, pl.ds(0, bins)]))
    field_in[own, :, pl.ds(bins, LANES)] = jnp.full((angles, LANES), 1.0, jnp.float32) * largest
    pl.semaphore_wait(barrier, 2 + line + jnp.where(line < lines - 1, 1, 0))

    def send(n, group, kind, slot, target):
        buffer = (index_in, field_in)[n]
        return pltpu.make_async_remote_copy(
            src_ref=buffer.at[group],
            dst_ref=buffer.at[group],
            send_sem=send_sems.at[n, kind, slot],
            recv_sem=recv_sems.at[n, group],
            device_id={"ang": target},
            device_id_type=pl.DeviceIdType.MESH,
        )

    def send_across(n, source):
        return send(n, 2 * source + column, 0, source, own ^ 1)

    def send_far(n, target):
        return send(n, own, 1, target, 2 * target + column)

    for target in range(lines - 2):

        @pl.when(target < line - 1)
        def _():
            pl.semaphore_signal(
                ready_sem, inc=1, device_id={"ang": 2 * target + column}, device_id_type=pl.DeviceIdType.MESH
            )

    for n in range(2):
        send_across(n, line).start()

        @pl.when(line < lines - 1)
        def _():
            send_far(n, line + 1).start()

        for target in range(lines - 1):

            @pl.when(target < line)
            def _():
                send_far(n, target).start()

    def send_late():
        @pl.when(lines - 2 - line > 0)
        def _():
            pl.semaphore_wait(ready_sem, lines - 2 - line)

        for n in range(2):
            for target in range(lines - 1, 1, -1):

                @pl.when(target > line + 1)
                def _():
                    send_far(n, target).start()

    edge = jnp.minimum(line, lines - 1 - line)

    def line_at(rank):
        inside = jnp.where(rank % 2 == 1, line - (rank + 1) // 2, line + rank // 2)
        outside = jnp.where(line < lines - 1 - line, rank, lines - 1 - rank)
        return jnp.where(rank <= 2 * edge, inside, outside)

    def source_at(place):
        rank = jnp.where(place < 2, 0, jnp.where(place <= lines, place - 1, place - lines))
        straight = jnp.logical_or(place == 0, jnp.logical_and(place >= 2, place <= lines))
        return line_at(rank), jnp.where(straight, column, 1 - column)

    def receive(n, place):
        source, side = source_at(place)
        group = 2 * source + side

        @pl.when(place > 0)
        def _():
            send(n, group, 0, 0, own ^ 1).wait_recv()

        @pl.when(jnp.logical_and(place >= 2, place <= lines))
        def _():
            send_across(n, source).start()

        return group

    def index_copies(group, side):
        outer = pl.multiple_of(bits[0] * (2 * LANES), LANES)
        for part, at in enumerate((LANES, outer)):
            yield pltpu.make_async_copy(
                index_in.at[group, :, pl.ds(at, LANES)], index_smem.at[side, part], smem_sems.at[side, part]
            )

    def prepare(group, side):
        peak = field_in[group, :, pl.ds(bins, LANES)]
        scale = TOP / jnp.maximum(peak, 1e-30)
        blocks = bins // LANES
        coded = []
        for block in range(blocks):
            value = field_in[group, :, pl.ds(block * LANES, LANES)]
            coded.append((value * scale + (TOP + 1.5)).astype(jnp.int32))
        for block in range(blocks):
            upper = jnp.left_shift(coded[(block + blocks // 2) % blocks] - int(TOP + 1), 16)
            packed = jnp.bitwise_or(upper, coded[block])
            for at in (block, block + blocks):
                if at < PITCH - 1:
                    table_ref[side, pl.ds(at, angles, stride=PITCH), :] = packed
        return peak * (1.0 / (TOP * math.sqrt(angles)))

    reverse_lane = LANES - 1 - lax.broadcasted_iota(jnp.int32, (SUBLANES, LANES), 1)
    samples_half = groups * width * ROW_PITCH

    middle = cuts[1] - cuts[0]

    def project(group, side, unit):
        start = (group ^ own) * (width * ROW_PITCH)
        for q in range(width):
            total = None
            upper = None
            for a in range(angles):
                code = index_smem[side, int(q >= middle), a, q if q < middle else q - middle]
                turn = jnp.bitwise_and(code, LANES - 1)
                base = jnp.right_shift(code, 7)
                near = table_ref[side, pl.ds(base, SUBLANES), :]
                next_ = table_ref[side, pl.ds(base + 1, SUBLANES), :]
                moved = pltpu.roll(jnp.where(reverse_lane < turn, near, next_), turn, 1)
                high = jnp.right_shift(moved, 16)
                total = moved if a == 0 else total + moved
                upper = high if a == 0 else upper + high
            lower = total - jnp.left_shift(upper, 16) - angles * int(TOP + 1)
            at = start + q * ROW_PITCH
            samples_ref[0, pl.ds(at, SUBLANES), :] = lower.astype(jnp.float32) * unit
            samples_ref[1, pl.ds(at, SUBLANES), :] = upper.astype(jnp.float32) * unit

    def prepare_weights():
        for load in loads[2:]:
            load.wait()
        parts = None
        for level in range(levels - 1, -1, -1):
            matrices = [merges[level, m] for m in range(2)]
            if level == 0:
                outer = [jnp.where(bits[0] == 1, m[:, cuts[1]:], m[:, : cuts[0]]) for m in matrices]
                matrices = [jnp.concatenate([m[:, cuts[0]:cuts[1]], o], axis=1) for m, o in zip(matrices, outer)]
            if parts is None:
                parts = matrices
            else:
                matrices = [split_bf16(m) for m in matrices]
                parts = [dot3(part, m) for part in [split_bf16(p) for p in parts] for m in matrices]
        flips = [int(format(k, f"0{levels}b")[::-1], 2) for k in range(groups)]
        whole = jnp.concatenate([parts[i] for i in flips], axis=1)
        weights_high[...], weights_low[...] = split_bf16(whole)

    for copy in index_copies(own, 0):
        copy.start()
    prepare_weights()

    def advance(place, side):
        last = place + 1 == groups

        @pl.when(place == 1)
        def _():
            send_late()
            for copy in index_copies(receive(0, place), side):
                copy.start()

        @pl.when(jnp.logical_and(place > 0, jnp.logical_not(last)))
        def _():
            for copy in index_copies(receive(0, place + 1), 1 - side):
                copy.start()

        group = receive(1, place)
        unit = prepare(group, side)
        for copy in index_copies(group, side):
            copy.wait()
        project(group, side, unit)

    def by_pairs(step, carry):
        advance(2 * step, 0)
        advance(2 * step + 1, 1)
        return carry

    lax.fori_loop(0, groups // 2, by_pairs, 0)

    depth = groups * width
    pairs = bins // (2 * LANES)

    def swap(n):
        at = pl.ds(pl.multiple_of(n * 2 * LANES, 2 * LANES), 2 * LANES)
        return pltpu.make_async_remote_copy(
            src_ref=out_ref.at[core, :, at],
            dst_ref=out_ref.at[core, :, at],
            send_sem=swap_send.at[n],
            recv_sem=swap_recv.at[n],
            device_id={"tile": seat ^ 1},
            device_id_type=pl.DeviceIdType.MESH,
        )

    def by_columns(n, carry):
        @pl.when(n > 0)
        def _():
            swap(n - 1).start()

        side = n // (pairs // 2)
        first = (n % (pairs // 2)) * 2
        parts = [samples_ref[side, pl.ds(first + i, depth, stride=ROW_PITCH), :] for i in range(2)]
        field = split_bf16(jnp.concatenate(parts, axis=1))
        total = dot3((weights_high[...], weights_low[...]), field)
        out_ref[core, :, pl.ds(pl.multiple_of(n * 2 * LANES, 2 * LANES), 2 * LANES)] = total
        return carry

    lax.fori_loop(0, pairs, by_columns, 0)
    swap(pairs - 1).start()
    for n in range(2):
        for source in range(lines):
            send_across(n, source).wait_send()

            @pl.when(source != line)
            def _():
                send_far(n, source).wait_send()

    for n in range(pairs):
        swap(n).wait()


def body(sinogram, ray_offsets, merge_matrices):
    slices, angles, bins = sinogram.shape
    rows = ray_offsets.shape[1]
    levels = merge_matrices.shape[0]
    groups = lax.axis_size("ang")
    assert slices == 2 and lax.axis_size("tile") % 2 == 0
    assert groups == 2**levels and angles == SUBLANES and bins == 2 * SUBLANES * LANES
    width = rows // 2 + rows // 8
    vmem = pl.BlockSpec(memory_space=pltpu.VMEM)
    hbm = pl.BlockSpec(memory_space=pltpu.HBM)
    dma = pltpu.SemaphoreType.DMA
    return pl.pallas_call(
        functools.partial(fused_kernel, (levels, angles, rows, bins)),
        out_shape=pltpu.VMEM((slices, rows, bins), jnp.float32),
        in_specs=[hbm, hbm, hbm],
        out_specs=vmem,
        scratch_shapes=[
            pltpu.VMEM((groups, angles, bins + LANES), jnp.float32),
            pltpu.VMEM((groups, angles, 3 * LANES), jnp.int32),
            pltpu.SMEM((2, 2, angles, LANES), jnp.int32),
            pltpu.VMEM((angles, rows), jnp.int32),
            pltpu.VMEM((levels, 2, rows, rows), jnp.float32),
            pltpu.VMEM((2, angles * PITCH, LANES), jnp.int32),
            pltpu.VMEM((2, groups * width * ROW_PITCH + SUBLANES, LANES), jnp.float32),
            pltpu.VMEM((rows, groups * width), jnp.bfloat16),
            pltpu.VMEM((rows, groups * width), jnp.bfloat16),
            dma((2 + levels,)),
            dma((2, 2)),
            dma((2, 2, groups // 2)),
            dma((2, groups)),
            pltpu.SemaphoreType.REGULAR,
            dma((bins // (2 * LANES),)),
            dma((bins // (2 * LANES),)),
        ],
        compiler_params=pltpu.CompilerParams(
            collective_id=0, has_side_effects=True, vmem_limit_bytes=48 * 1024 * 1024
        ),
    )(*[pltpu.with_memory_space_constraint(x, pltpu.HBM) for x in (sinogram, ray_offsets, merge_matrices)])


def solution(mesh):
    placed = (P(None, "ang", None), P("ang", None), P())
    return jax.shard_map(
        body, mesh=mesh, in_specs=placed, out_specs=P(None, "ang", None), check_vma=False
    )
```

```python
import functools
import math

import jax
import jax.numpy as jnp
from jax import lax
from jax.experimental import pallas as pl
from jax.experimental.pallas import tpu as pltpu
from jax.sharding import PartitionSpec as P

LANES = 128
SUBLANES = 8
PITCH = 3 * SUBLANES + 1
ROW_PITCH = SUBLANES + 4
TOP = 32767.0


def split_bf16(value):
    high = value.astype(jnp.bfloat16)
    return high, (value - high.astype(jnp.float32)).astype(jnp.bfloat16)


def dot3(left, right):
    dot = functools.partial(jnp.dot, preferred_element_type=jnp.float32)
    return dot(left[0], right[0]) + (dot(left[0], right[1]) + dot(left[1], right[0]))


def fused_kernel(dims, sino_ref, offsets_ref, merge_ref, out_ref, field_in, index_in, index_smem, offsets, merges, table_ref,
                 samples_ref, weights_high, weights_low, in_sems, smem_sems, send_sems, recv_sems, ready_sem, swap_send, swap_recv):
    levels, angles, rows, bins = dims
    groups = 2**levels
    lines = groups // 2
    cuts = (rows // 2 - rows // 8, rows // 2 + rows // 8)
    width = cuts[1]
    own = lax.axis_index("ang")
    line, column = lax.div(own, 2), lax.rem(own, 2)
    seat = lax.axis_index("tile")
    core = lax.rem(seat, 2)
    bits = [lax.rem(lax.div(own, 2 ** (levels - 1 - level)), 2) for level in range(levels)]

    barrier = pltpu.get_barrier_semaphore()

    def greet(peer):
        pl.semaphore_signal(barrier, inc=1, device_id=peer, device_id_type=pl.DeviceIdType.MESH)

    greet({"ang": own ^ 1})
    greet({"tile": seat ^ 1})

    @pl.when(line > 0)
    def _():
        greet({"ang": own - 2})

    for step in range(1, lines):

        @pl.when(line + step < lines)
        def _():
            greet({"ang": own + 2 * step})

    loads = [
        pltpu.make_async_copy(sino_ref.at[core], field_in.at[own, :, pl.ds(0, bins)], in_sems.at[0]),
        pltpu.make_async_copy(offsets_ref, offsets, in_sems.at[1]),
    ]
    for level in range(levels):
        loads.append(pltpu.make_async_copy(merge_ref.at[level, bits[level]], merges.at[level], in_sems.at[2 + level]))
    for load in loads:
        load.start()
    loads[1].wait()
    place_code = lax.broadcasted_iota(jnp.int32, (angles, rows), 0) * (PITCH * LANES)
    codes = (jnp.bitwise_and(offsets[...] + (bins - 1), bins - 1) ^ (LANES - 1)) + place_code
    for part, (first, last) in enumerate(((0, cuts[0]), cuts, (cuts[1], rows))):
        index_in[own, :, pl.ds(part * LANES, last - first)] = codes[:, first:last]
    loads[0].wait()
    largest = jnp.max(jnp.abs(field_in[own, :, pl.ds(0, bins)]))
    field_in[own, :, pl.ds(bins, LANES)] = jnp.full((angles, LANES), 1.0, jnp.float32) * largest
    pl.semaphore_wait(barrier, 2 + line + jnp.where(line < lines - 1, 1, 0))

    def send(n, group, kind, slot, target):
        buffer = (index_in, field_in)[n]
        return pltpu.make_async_remote_copy(
            src_ref=buffer.at[group],
            dst_ref=buffer.at[group],
            send_sem=send_sems.at[n, kind, slot],
            recv_sem=recv_sems.at[n, group],
            device_id={"ang": target},
            device_id_type=pl.DeviceIdType.MESH,
        )

    def send_across(n, source):
        return send(n, 2 * source + column, 0, source, own ^ 1)

    def send_far(n, target):
        return send(n, own, 1, target, 2 * target + column)

    for target in range(lines - 2):

        @pl.when(target < line - 1)
        def _():
            pl.semaphore_signal(
                ready_sem, inc=1, device_id={"ang": 2 * target + column}, device_id_type=pl.DeviceIdType.MESH
            )

    for n in range(2):
        send_across(n, line).start()

        @pl.when(line < lines - 1)
        def _():
            send_far(n, line + 1).start()

        for target in range(lines - 1):

            @pl.when(target < line)
            def _():
                send_far(n, target).start()

    def send_late():
        @pl.when(lines - 2 - line > 0)
        def _():
            pl.semaphore_wait(ready_sem, lines - 2 - line)

        for n in range(2):
            for target in range(lines - 1, 1, -1):

                @pl.when(target > line + 1)
                def _():
                    send_far(n, target).start()

    edge = jnp.minimum(line, lines - 1 - line)

    def line_at(rank):
        inside = jnp.where(rank % 2 == 1, line - (rank + 1) // 2, line + rank // 2)
        outside = jnp.where(line < lines - 1 - line, rank, lines - 1 - rank)
        return jnp.where(rank <= 2 * edge, inside, outside)

    def source_at(place):
        rank = jnp.where(place < 2, 0, jnp.where(place <= lines, place - 1, place - lines))
        straight = jnp.logical_or(place == 0, jnp.logical_and(place >= 2, place <= lines))
        return line_at(rank), jnp.where(straight, column, 1 - column)

    def receive(n, place):
        source, side = source_at(place)
        group = 2 * source + side

        @pl.when(place > 0)
        def _():
            send(n, group, 0, 0, own ^ 1).wait_recv()

        @pl.when(jnp.logical_and(place >= 2, place <= lines))
        def _():
            send_across(n, source).start()

        return group

    def index_copies(group, side):
        outer = pl.multiple_of(bits[0] * (2 * LANES), LANES)
        for part, at in enumerate((LANES, outer)):
            yield pltpu.make_async_copy(
                index_in.at[group, :, pl.ds(at, LANES)], index_smem.at[side, part], smem_sems.at[side, part]
            )

    def prepare(group, side):
        peak = field_in[group, :, pl.ds(bins, LANES)]
        scale = TOP / jnp.maximum(peak, 1e-30)
        blocks = bins // LANES
        coded = []
        for block in range(blocks):
            value = field_in[group, :, pl.ds(block * LANES, LANES)]
            coded.append((value * scale + (TOP + 1.5)).astype(jnp.int32))
        for block in range(blocks):
            upper = jnp.left_shift(coded[(block + blocks // 2) % blocks] - int(TOP + 1), 16)
            packed = jnp.bitwise_or(upper, coded[block])
            for at in (block, block + blocks):
                if at < PITCH - 1:
                    table_ref[side, pl.ds(at, angles, stride=PITCH), :] = packed
        return peak * (1.0 / (TOP * math.sqrt(angles)))

    reverse_lane = LANES - 1 - lax.broadcasted_iota(jnp.int32, (SUBLANES, LANES), 1)

    middle = cuts[1] - cuts[0]

    pairs = bins // (2 * LANES)

    def project(side, unit, between):
        for q in range(width):
            if q % (width // pairs) == 0:
                between(q // (width // pairs))
            total = None
            upper = None
            for a in range(angles):
                code = index_smem[side, int(q >= middle), a, q if q < middle else q - middle]
                turn = jnp.bitwise_and(code, LANES - 1)
                base = jnp.right_shift(code, 7)
                near = table_ref[side, pl.ds(base, SUBLANES), :]
                next_ = table_ref[side, pl.ds(base + 1, SUBLANES), :]
                moved = pltpu.roll(jnp.where(reverse_lane < turn, near, next_), turn, 1)
                high = jnp.right_shift(moved, 16)
                total = moved if a == 0 else total + moved
                upper = high if a == 0 else upper + high
            lower = total - jnp.left_shift(upper, 16) - angles * int(TOP + 1)
            at = q * ROW_PITCH
            samples_ref[side, 0, pl.ds(at, SUBLANES), :] = lower.astype(jnp.float32) * unit
            samples_ref[side, 1, pl.ds(at, SUBLANES), :] = upper.astype(jnp.float32) * unit

    def prepare_weights():
        parts = None
        for level in range(levels - 1, -1, -1):
            matrices = [merges[level, m] for m in range(2)]
            if level == 0:
                outer = [jnp.where(bits[0] == 1, m[:, cuts[1]:], m[:, : cuts[0]]) for m in matrices]
                matrices = [jnp.concatenate([m[:, cuts[0]:cuts[1]], o], axis=1) for m, o in zip(matrices, outer)]
            if parts is None:
                parts = matrices
            else:
                matrices = [split_bf16(m) for m in matrices]
                parts = [dot3(part, m) for part in [split_bf16(p) for p in parts] for m in matrices]
        flips = [int(format(k, f"0{levels}b")[::-1], 2) for k in range(groups)]
        for k, i in enumerate(flips):
            weights_high[k], weights_low[k] = split_bf16(parts[i])

    def merge(place, side, n):
        source, column_side = source_at(place)
        k = (2 * source + column_side) ^ own
        parts = [samples_ref[side, n // (pairs // 2), pl.ds((n % (pairs // 2)) * 2 + i, width, stride=ROW_PITCH), :] for i in range(2)]
        field = split_bf16(jnp.concatenate(parts, axis=1))
        at = pl.ds(n * 2 * LANES, 2 * LANES)
        out_ref[core, :, at] += dot3((weights_high[k], weights_low[k]), field)

    for copy in index_copies(own, 0):
        copy.start()
    unit = prepare(own, 0)
    for load in loads[2:]:
        load.wait()
    out_ref[core] = jnp.zeros((rows, bins), jnp.float32)
    prepare_weights()
    for copy in index_copies(own, 0):
        copy.wait()
    project(0, unit, lambda n: None)
    send_late()
    for copy in index_copies(receive(0, 1), 1):
        copy.start()

    def advance(place, side):
        @pl.when(place + 1 < groups)
        def _():
            for copy in index_copies(receive(0, place + 1), 1 - side):
                copy.start()

        group = receive(1, place)
        unit = prepare(group, side)
        for copy in index_copies(group, side):
            copy.wait()
        project(side, unit, lambda n: merge(place - 1, 1 - side, n))

    def by_pairs(step, carry):
        advance(2 * step + 1, 1)
        advance(2 * step + 2, 0)
        return carry

    lax.fori_loop(0, groups // 2 - 1, by_pairs, 0)
    advance(groups - 1, 1)

    chunks = pairs // 2

    def swap(n):
        at = pl.ds(n * (bins // chunks), bins // chunks)
        return pltpu.make_async_remote_copy(
            src_ref=out_ref.at[core, :, at],
            dst_ref=out_ref.at[core, :, at],
            send_sem=swap_send.at[n],
            recv_sem=swap_recv.at[n],
            device_id={"tile": seat ^ 1},
            device_id_type=pl.DeviceIdType.MESH,
        )

    for n in range(2):
        for source in range(lines):
            send_across(n, source).wait_send()

            @pl.when(source != line)
            def _():
                send_far(n, source).wait_send()

    for n in range(chunks):
        for tile in range(pairs // chunks):
            merge(groups - 1, 1, n * (pairs // chunks) + tile)
        swap(n).start()
    for n in range(chunks):
        swap(n).wait()


def body(sinogram, ray_offsets, merge_matrices):
    slices, angles, bins = sinogram.shape
    rows = ray_offsets.shape[1]
    levels = merge_matrices.shape[0]
    groups = lax.axis_size("ang")
    assert slices == 2 and lax.axis_size("tile") % 2 == 0
    assert groups == 2**levels and angles == SUBLANES and bins == 2 * SUBLANES * LANES
    width = rows // 2 + rows // 8
    vmem = pl.BlockSpec(memory_space=pltpu.VMEM)
    hbm = pl.BlockSpec(memory_space=pltpu.HBM)
    dma = pltpu.SemaphoreType.DMA
    return pl.pallas_call(
        functools.partial(fused_kernel, (levels, angles, rows, bins)),
        out_shape=pltpu.VMEM((slices, rows, bins), jnp.float32),
        in_specs=[hbm, hbm, hbm],
        out_specs=vmem,
        scratch_shapes=[
            pltpu.VMEM((groups, angles, bins + LANES), jnp.float32),
            pltpu.VMEM((groups, angles, 3 * LANES), jnp.int32),
            pltpu.SMEM((2, 2, angles, LANES), jnp.int32),
            pltpu.VMEM((angles, rows), jnp.int32),
            pltpu.VMEM((levels, 2, rows, rows), jnp.float32),
            pltpu.VMEM((2, angles * PITCH, LANES), jnp.int32),
            pltpu.VMEM((2, 2, width * ROW_PITCH, LANES), jnp.float32),
            pltpu.VMEM((groups, rows, width), jnp.bfloat16),
            pltpu.VMEM((groups, rows, width), jnp.bfloat16),
            dma((2 + levels,)),
            dma((2, 2)),
            dma((2, 2, groups // 2)),
            dma((2, groups)),
            pltpu.SemaphoreType.REGULAR,
            dma((bins // (4 * LANES),)),
            dma((bins // (4 * LANES),)),
        ],
        compiler_params=pltpu.CompilerParams(
            collective_id=0, has_side_effects=True, vmem_limit_bytes=48 * 1024 * 1024
        ),
    )(*[pltpu.with_memory_space_constraint(x, pltpu.HBM) for x in (sinogram, ray_offsets, merge_matrices)])


def solution(mesh):
    placed = (P(None, "ang", None), P("ang", None), P())
    return jax.shard_map(
        body, mesh=mesh, in_specs=placed, out_specs=P(None, "ang", None), check_vma=False
    )
```

```python
import functools
import math

import jax
import jax.numpy as jnp
from jax import lax
from jax.experimental import pallas as pl
from jax.experimental.pallas import tpu as pltpu
from jax.sharding import PartitionSpec as P

LANES = 128
SUBLANES = 8
PITCH = 3 * SUBLANES + 1
ROW_PITCH = SUBLANES + 4
TOP = 32767.0


def split_bf16(value):
    high = value.astype(jnp.bfloat16)
    return high, (value - high.astype(jnp.float32)).astype(jnp.bfloat16)


def dot3(left, right):
    dot = functools.partial(jnp.dot, preferred_element_type=jnp.float32)
    return dot(left[0], right[0]) + (dot(left[0], right[1]) + dot(left[1], right[0]))


def fused_kernel(dims, sino_ref, offsets_ref, merge_ref, out_ref, field_in, index_in, index_smem, offsets, merges, table_ref,
                 samples_ref, weights_high, weights_low, in_sems, smem_sems, send_sems, recv_sems, ready_sem, swap_send, swap_recv):
    levels, angles, rows, bins = dims
    groups = 2**levels
    lines = groups // 2
    cuts = (rows // 2 - rows // 8, rows // 2 + rows // 8)
    width = cuts[1]
    own = lax.axis_index("ang")
    line, column = lax.div(own, 2), lax.rem(own, 2)
    seat = lax.axis_index("tile")
    core = lax.rem(seat, 2)
    bits = [lax.rem(lax.div(own, 2 ** (levels - 1 - level)), 2) for level in range(levels)]

    barrier = pltpu.get_barrier_semaphore()

    def greet(peer):
        pl.semaphore_signal(barrier, inc=1, device_id=peer, device_id_type=pl.DeviceIdType.MESH)

    greet({"ang": own ^ 1})
    greet({"tile": seat ^ 1})

    @pl.when(line > 0)
    def _():
        greet({"ang": own - 2})

    for step in range(1, lines):

        @pl.when(line + step < lines)
        def _():
            greet({"ang": own + 2 * step})

    loads = [
        pltpu.make_async_copy(sino_ref.at[core], field_in.at[own, :, pl.ds(0, bins)], in_sems.at[0]),
        pltpu.make_async_copy(offsets_ref, offsets, in_sems.at[1]),
    ]
    for level in range(levels):
        loads.append(pltpu.make_async_copy(merge_ref.at[level, bits[level]], merges.at[level], in_sems.at[2 + level]))
    for load in loads:
        load.start()
    loads[1].wait()
    place_code = lax.broadcasted_iota(jnp.int32, (angles, rows), 0) * (PITCH * LANES)
    codes = (jnp.bitwise_and(offsets[...] + (bins - 1), bins - 1) ^ (LANES - 1)) + place_code
    for part, (first, last) in enumerate(((0, cuts[0]), cuts, (cuts[1], rows))):
        index_in[own, :, pl.ds(part * LANES, last - first)] = codes[:, first:last]
    loads[0].wait()
    largest = jnp.max(jnp.abs(field_in[own, :, pl.ds(0, bins)]))
    field_in[own, :, pl.ds(bins, LANES)] = jnp.full((angles, LANES), 1.0, jnp.float32) * largest
    pl.semaphore_wait(barrier, 2 + line + jnp.where(line < lines - 1, 1, 0))

    def send(n, group, kind, slot, target):
        buffer = (index_in, field_in)[n]
        return pltpu.make_async_remote_copy(
            src_ref=buffer.at[group],
            dst_ref=buffer.at[group],
            send_sem=send_sems.at[n, kind, slot],
            recv_sem=recv_sems.at[n, group],
            device_id={"ang": target},
            device_id_type=pl.DeviceIdType.MESH,
        )

    def send_across(n, source):
        return send(n, 2 * source + column, 0, source, own ^ 1)

    def send_far(n, target):
        return send(n, own, 1, target, 2 * target + column)

    for target in range(lines - 2):

        @pl.when(target < line - 1)
        def _():
            pl.semaphore_signal(
                ready_sem, inc=1, device_id={"ang": 2 * target + column}, device_id_type=pl.DeviceIdType.MESH
            )

    def is_held(n, target):
        return jnp.logical_and(line > lines // 2, n * (line - target) >= 2)

    ahead = jnp.logical_and(line >= lines // 2, line < lines - 1)

    for n in range(2):

        @pl.when(ahead)
        def _():
            send_far(n, 0).start()

        send_across(n, line).start()

        for target in range(lines - 1):
            starts = jnp.logical_and(target < line, jnp.logical_not(is_held(n, target)))
            if target == 0:
                starts = jnp.logical_and(starts, jnp.logical_not(ahead))

            @pl.when(starts)
            def _():
                send_far(n, target).start()

        @pl.when(line < lines - 1)
        def _():
            send_far(n, line + 1).start()

    def send_held():
        for target in range(lines - 2):

            held = is_held(1, target)
            if target == 0:
                held = jnp.logical_and(held, jnp.logical_not(ahead))

            @pl.when(held)
            def _():
                send_far(1, target).start()

    def send_late():
        @pl.when(lines - 2 - line > 0)
        def _():
            pl.semaphore_wait(ready_sem, lines - 2 - line)

        for n in range(2):
            for target in range(lines - 1, 1, -1):

                @pl.when(target > line + 1)
                def _():
                    send_far(n, target).start()

    edge = jnp.minimum(line, lines - 1 - line)

    def line_at(rank):
        inside = jnp.where(rank % 2 == 1, line - (rank + 1) // 2, line + rank // 2)
        outside = jnp.where(line < lines - 1 - line, rank, lines - 1 - rank)
        return jnp.where(rank <= 2 * edge, inside, outside)

    def source_at(place):
        rank = jnp.where(place < 2, 0, jnp.where(place <= lines, place - 1, place - lines))
        straight = jnp.logical_or(place == 0, jnp.logical_and(place >= 2, place <= lines))
        return line_at(rank), jnp.where(straight, column, 1 - column)

    def receive(n, place):
        source, side = source_at(place)
        group = 2 * source + side

        @pl.when(place > 0)
        def _():
            send(n, group, 0, 0, own ^ 1).wait_recv()

        @pl.when(jnp.logical_and(place >= 2, place <= lines))
        def _():
            send_across(n, source).start()

        return group

    def index_copies(group, side):
        outer = pl.multiple_of(bits[0] * (2 * LANES), LANES)
        for part, at in enumerate((LANES, outer)):
            yield pltpu.make_async_copy(
                index_in.at[group, :, pl.ds(at, LANES)], index_smem.at[side, part], smem_sems.at[side, part]
            )

    def prepare(group, side):
        peak = field_in[group, :, pl.ds(bins, LANES)]
        scale = TOP / jnp.maximum(peak, 1e-30)
        blocks = bins // LANES
        coded = []
        for block in range(blocks):
            value = field_in[group, :, pl.ds(block * LANES, LANES)]
            coded.append((value * scale + (TOP + 1.5)).astype(jnp.int32))
        for block in range(blocks):
            upper = jnp.left_shift(coded[(block + blocks // 2) % blocks] - int(TOP + 1), 16)
            packed = jnp.bitwise_or(upper, coded[block])
            for at in (block, block + blocks):
                if at < PITCH - 1:
                    table_ref[side, pl.ds(at, angles, stride=PITCH), :] = packed
        return peak * (1.0 / (TOP * math.sqrt(angles)))

    reverse_lane = LANES - 1 - lax.broadcasted_iota(jnp.int32, (SUBLANES, LANES), 1)

    middle = cuts[1] - cuts[0]

    pairs = bins // (2 * LANES)

    def project(side, unit, between):
        for q in range(width):
            if q % (width // pairs) == 0:
                between(q // (width // pairs))
            total = None
            upper = None
            for a in range(angles):
                code = index_smem[side, int(q >= middle), a, q if q < middle else q - middle]
                turn = jnp.bitwise_and(code, LANES - 1)
                base = jnp.right_shift(code, 7)
                near = table_ref[side, pl.ds(base, SUBLANES), :]
                next_ = table_ref[side, pl.ds(base + 1, SUBLANES), :]
                moved = pltpu.roll(jnp.where(reverse_lane < turn, near, next_), turn, 1)
                high = jnp.right_shift(moved, 16)
                total = moved if a == 0 else total + moved
                upper = high if a == 0 else upper + high
            lower = total - jnp.left_shift(upper, 16) - angles * int(TOP + 1)
            at = q * ROW_PITCH
            samples_ref[side, 0, pl.ds(at, SUBLANES), :] = lower.astype(jnp.float32) * unit
            samples_ref[side, 1, pl.ds(at, SUBLANES), :] = upper.astype(jnp.float32) * unit

    def prepare_weights():
        parts = None
        for level in range(levels - 1, -1, -1):
            matrices = [merges[level, m] for m in range(2)]
            if level == 0:
                outer = [jnp.where(bits[0] == 1, m[:, cuts[1]:], m[:, : cuts[0]]) for m in matrices]
                matrices = [jnp.concatenate([m[:, cuts[0]:cuts[1]], o], axis=1) for m, o in zip(matrices, outer)]
            if parts is None:
                parts = matrices
            else:
                matrices = [split_bf16(m) for m in matrices]
                parts = [dot3(part, m) for part in [split_bf16(p) for p in parts] for m in matrices]
        flips = [int(format(k, f"0{levels}b")[::-1], 2) for k in range(groups)]
        for k, i in enumerate(flips):
            weights_high[k], weights_low[k] = split_bf16(parts[i])

    def merge(place, side, n):
        source, column_side = source_at(place)
        k = (2 * source + column_side) ^ own
        parts = [samples_ref[side, n // (pairs // 2), pl.ds((n % (pairs // 2)) * 2 + i, width, stride=ROW_PITCH), :] for i in range(2)]
        field = split_bf16(jnp.concatenate(parts, axis=1))
        at = pl.ds(n * 2 * LANES, 2 * LANES)
        out_ref[core, :, at] += dot3((weights_high[k], weights_low[k]), field)

    for copy in index_copies(own, 0):
        copy.start()
    unit = prepare(own, 0)
    for load in loads[2:]:
        load.wait()
    out_ref[core] = jnp.zeros((rows, bins), jnp.float32)
    prepare_weights()
    send_held()
    for copy in index_copies(own, 0):
        copy.wait()
    project(0, unit, lambda n: None)
    send_late()
    for copy in index_copies(receive(0, 1), 1):
        copy.start()

    def advance(place, side):
        @pl.when(place + 1 < groups)
        def _():
            for copy in index_copies(receive(0, place + 1), 1 - side):
                copy.start()

        group = receive(1, place)
        unit = prepare(group, side)
        for copy in index_copies(group, side):
            copy.wait()
        project(side, unit, lambda n: merge(place - 1, 1 - side, n))

    def by_pairs(step, carry):
        advance(2 * step + 1, 1)
        advance(2 * step + 2, 0)
        return carry

    lax.fori_loop(0, groups // 2 - 1, by_pairs, 0)
    advance(groups - 1, 1)

    chunks = pairs // 2

    def swap(n):
        at = pl.ds(n * (bins // chunks), bins // chunks)
        return pltpu.make_async_remote_copy(
            src_ref=out_ref.at[core, :, at],
            dst_ref=out_ref.at[core, :, at],
            send_sem=swap_send.at[n],
            recv_sem=swap_recv.at[n],
            device_id={"tile": seat ^ 1},
            device_id_type=pl.DeviceIdType.MESH,
        )

    for n in range(2):
        for source in range(lines):
            send_across(n, source).wait_send()

            @pl.when(source != line)
            def _():
                send_far(n, source).wait_send()

    for n in range(chunks):
        for tile in range(pairs // chunks):
            merge(groups - 1, 1, n * (pairs // chunks) + tile)
        swap(n).start()
    for n in range(chunks):
        swap(n).wait()


def body(sinogram, ray_offsets, merge_matrices):
    slices, angles, bins = sinogram.shape
    rows = ray_offsets.shape[1]
    levels = merge_matrices.shape[0]
    groups = lax.axis_size("ang")
    assert slices == 2 and lax.axis_size("tile") % 2 == 0
    assert groups == 2**levels and angles == SUBLANES and bins == 2 * SUBLANES * LANES
    width = rows // 2 + rows // 8
    vmem = pl.BlockSpec(memory_space=pltpu.VMEM)
    hbm = pl.BlockSpec(memory_space=pltpu.HBM)
    dma = pltpu.SemaphoreType.DMA
    return pl.pallas_call(
        functools.partial(fused_kernel, (levels, angles, rows, bins)),
        out_shape=pltpu.VMEM((slices, rows, bins), jnp.float32),
        in_specs=[hbm, hbm, hbm],
        out_specs=vmem,
        scratch_shapes=[
            pltpu.VMEM((groups, angles, bins + LANES), jnp.float32),
            pltpu.VMEM((groups, angles, 3 * LANES), jnp.int32),
            pltpu.SMEM((2, 2, angles, LANES), jnp.int32),
            pltpu.VMEM((angles, rows), jnp.int32),
            pltpu.VMEM((levels, 2, rows, rows), jnp.float32),
            pltpu.VMEM((2, angles * PITCH, LANES), jnp.int32),
            pltpu.VMEM((2, 2, width * ROW_PITCH, LANES), jnp.float32),
            pltpu.VMEM((groups, rows, width), jnp.bfloat16),
            pltpu.VMEM((groups, rows, width), jnp.bfloat16),
            dma((2 + levels,)),
            dma((2, 2)),
            dma((2, 2, groups // 2)),
            dma((2, groups)),
            pltpu.SemaphoreType.REGULAR,
            dma((bins // (4 * LANES),)),
            dma((bins // (4 * LANES),)),
        ],
        compiler_params=pltpu.CompilerParams(
            collective_id=0, has_side_effects=True, vmem_limit_bytes=48 * 1024 * 1024
        ),
    )(*[pltpu.with_memory_space_constraint(x, pltpu.HBM) for x in (sinogram, ray_offsets, merge_matrices)])


def solution(mesh):
    placed = (P(None, "ang", None), P("ang", None), P())
    return jax.shard_map(
        body, mesh=mesh, in_specs=placed, out_specs=P(None, "ang", None), check_vma=False
    )
```
